512 devices in a mesh: dp: 128 (over z, x, core), mp: 4 (over y).
Axes of the slice: x: 4, y: 4, z: 16, core: 2. Of those that a mesh axis runs over, the one named last changes fastest.
Arguments:
- grad_blocks: bfloat16 [256, 128, 128], P('dp', None, 'mp'), may hold values from -0.5 to 0.5
- owner_table: int32 [256], replicated, may hold values from 0 to 127, as said below
- prev_stats: float32 [1024, 2, 128, 128], P('dp'), as said below
Outputs:
- update: bfloat16 [256, 128, 128], P('dp', None, 'mp')
- new_stats: float32 [1024, 2, 128, 128], P('dp')
- inv_roots: float32 [1024, 2, 128, 128], P('dp')
The draws below stay inside these ranges and needn't reach their ends.
Inputs may be any that keep to these rules, and one draw needn't show every extreme that they name: `owner_table`: every entry is a dp index; no index appears more than 8 times, and some index appears exactly 8 times. `prev_stats`: each [128, 128] matrix is symmetric positive semidefinite.
All inputs are finite; a program needn't handle non-finite values.
Results may differ from the reference program's by a relative error of at most 0.001.
Values may be sent and summed in bfloat16 or wider, within the bound.
A program may use at most 64 MiB of HBM per device.

```python
import jax
import jax.numpy as jnp
from jax import lax

BLOCK = 128
BLK_DEV = 2
ITERS = 16
NBLK = 256
CAP = 8
N_DP = 128


def draw_owner_table(key, part):
    dev_count = NBLK // BLK_DEV
    slot_count = dev_count * CAP
    base = jax.random.fold_in(key, 17)
    key_bias, key_noise, key_pick, key_order = jax.random.split(base, 4)
    weights = jax.random.randint(key_bias, (dev_count,), 0, 2).astype(jnp.int32)
    noise = jax.random.randint(key_noise, (slot_count,), 0, 2048).astype(jnp.int32)
    favored = jax.random.randint(key_pick, (), 0, dev_count).astype(jnp.int32)
    slot_range = jnp.arange(slot_count, dtype=jnp.int32)
    slot_owner = slot_range // CAP
    forced = (slot_range == 0) | (slot_range == (dev_count - 1) * CAP)
    score = weights[slot_owner] * 1024 + noise + jnp.where(slot_owner == favored, 8192, 0).astype(jnp.int32)
    score = score + jnp.where(forced, 16384, 0).astype(jnp.int32)
    score = score * slot_count + slot_range
    unused_vals, chosen = lax.top_k(score, NBLK)
    shuffled = jax.random.permutation(key_order, chosen)
    return (shuffled // CAP).astype(jnp.int32)


def draw_prev_stats(key, part):
    dev_count = NBLK // BLK_DEV
    count = dev_count * CAP * 2
    base = jax.random.fold_in(key, 29)
    key_mat, key_scale = jax.random.split(base, 2)
    factors = jax.random.normal(key_mat, (count, BLOCK, BLOCK), jnp.float32)
    product = jnp.einsum('pik,pjk->pij', factors, factors) / BLOCK
    product = 0.5 * (product + jnp.swapaxes(product, 1, 2))
    return product.reshape(dev_count * CAP, 2, BLOCK, BLOCK).astype(jnp.float32)


def shard_levels(stream_key, extent, cuts, low, largest):
    gain, own = 1.0, jax.random.fold_in(stream_key, 6)
    for dim, blocks in cuts:
        steps = jnp.exp(jax.random.uniform(jax.random.fold_in(own, dim), (blocks,), jnp.float32, low / len(cuts), largest / len(cuts)))
        gain = gain * jnp.repeat(steps, extent[dim] // blocks).reshape([-1 if axis == dim else 1 for axis in range(len(extent))])
    return gain


def centred(stream_key, dims, scale, limit, shards=(), kind=jnp.bfloat16):
    drawn = jax.random.normal(stream_key, dims, jnp.float32) * scale
    if len(shards) > 0:
        drawn = shard_levels(stream_key, dims, shards, -0.22, 0.18) * drawn
    return jnp.clip(drawn, min=-limit, max=limit).astype(kind)


def setup_inputs(seed: int = 0) -> dict:
    splits = jax.random.split(jax.random.key(seed), 4)
    grad_blocks = centred(splits[0], (NBLK, BLOCK, BLOCK), BLOCK ** -0.5, 0.5, ((0, 128), (2, 4)))
    owner_table = draw_owner_table(jax.random.fold_in(splits[3], 71), 0)
    prev_stats = draw_prev_stats(jax.random.fold_in(splits[3], 71), 0)
    return dict(grad_blocks=grad_blocks, owner_table=owner_table, prev_stats=prev_stats)


STAT_DECAY = 0.75
DAMPING = 0.03

def batch_product(first, second):
    return jnp.einsum('pij,pjk->pik', first, second, precision=lax.Precision.HIGHEST)

def newton_roots(matrices):
    width = matrices.shape[-1]
    identity = jnp.eye(width, dtype=jnp.float32)
    trace_val = jnp.trace(matrices, axis1=1, axis2=2)
    damped = matrices + DAMPING / width * trace_val[:, None, None] * identity
    norm_val = jnp.sqrt(lax.optimization_barrier(jnp.sum(damped * damped, axis=(1, 2))))
    root_mat = identity * (1.0 / jnp.sqrt(jnp.sqrt(norm_val)))[:, None, None]
    remainder = damped / norm_val[:, None, None]

    def refine(unused, state_pair):
        root_now, rest_now = state_pair
        factor = (5.0 * identity - rest_now) * 0.25
        root_now = batch_product(root_now, factor)
        square = batch_product(factor, factor)
        quartic = batch_product(square, square)
        return (root_now, batch_product(quartic, rest_now))
    root_mat, remainder = lax.fori_loop(0, ITERS, refine, (root_mat, remainder))
    return root_mat

def reference(grad_blocks, owner_table, prev_stats):
    grad_wide = grad_blocks.astype(jnp.float32)
    left_stat = jnp.einsum('bik,bjk->bij', grad_wide, grad_wide, precision=lax.Precision.HIGHEST)
    right_stat = jnp.einsum('bki,bkj->bij', grad_wide, grad_wide, precision=lax.Precision.HIGHEST)
    owners_hot = (owner_table[:, None] == jnp.arange(N_DP, dtype=jnp.int32)[None, :]).astype(jnp.int32)
    earlier = jnp.cumsum(owners_hot, axis=0) - owners_hot
    slot_rank = lax.optimization_barrier(jnp.sum(earlier * owners_hot, axis=1))
    slot_ids = (owner_table * CAP + slot_rank).astype(jnp.int32)
    previous = prev_stats[slot_ids]
    blended = STAT_DECAY * previous + (1.0 - STAT_DECAY) * jnp.stack([left_stat, right_stat], axis=1)
    roots = lax.map(newton_roots, blended)
    precond = jnp.einsum('bij,bjk->bik', roots[:, 0], grad_wide, precision=lax.Precision.HIGHEST)
    precond = jnp.einsum('bij,bjk->bik', precond, roots[:, 1], precision=lax.Precision.HIGHEST)
    spread = jnp.sqrt(lax.optimization_barrier(jnp.mean(precond * precond, axis=(1, 2))))
    update = (precond / spread[:, None, None]).astype(jnp.bfloat16)
    empty = jnp.zeros((N_DP * CAP, 2, BLOCK, BLOCK), jnp.float32)
    new_stats = empty.at[slot_ids].set(blended)
    inv_roots = empty.at[slot_ids].set(roots)
    return (update, new_stats, inv_roots)
```

```python
import jax
import jax.numpy as jnp
from jax import lax
from jax.experimental import pallas as pl
from jax.experimental.pallas import tpu as pltpu
from jax.sharding import PartitionSpec as P

ITERS = 16
STAT_DECAY = 0.75
DAMPING = 0.03
N = 128
XS, CORES, YS = 4, 2, 4
CAP = 8
NEAR = 4
MESH = pl.DeviceIdType.MESH
BF = jnp.bfloat16
F32 = jnp.float32


def split(a):
    hi = a.astype(BF)
    return hi, (a - hi.astype(F32)).astype(BF)


def wide(a):
    return jnp.concatenate(split(a), axis=1)


def tall(a):
    row = wide(a)
    return jnp.concatenate([row, row], axis=0)


def product(left, right):
    out = jnp.dot(left, right, preferred_element_type=F32)
    return out[:, :N] + out[:, N:]


def kernel(
    zs,
    grad_ref, owner_ref, prev_ref,
    upd_ref, stats_ref, roots_ref,
    zbuf, sel1, rbuf, gt, prev, stat, root, mstate, xstate, ubuf, vbuf, wbuf, bfar, mfar, abuf, tabv, tabs,
    z_send, z_recv, d_send, d_recv, p_send, p_recv, s_send, s_recv, r_send, r_recv,
    u_send, u_recv, e_send, e_recv, w_send, w_recv, loc,
):
    dp = lax.axis_index("dp")
    q = lax.axis_index("mp")
    z = lax.div(dp, XS * CORES)
    x = lax.rem(lax.div(dp, CORES), XS)
    c = lax.rem(dp, CORES)

    def zoff(d):
        return lax.rem(z + (d + zs), zs)

    def dev(zz, xx, cc, yy):
        return ((zz * XS + xx) * CORES + cc, yy)

    def along(d):
        return dev(zoff(d), x, c, q)

    def plane(dx, dy):
        return lax.rem(x + dx, XS), lax.rem(q + dy, YS)

    other = dev(z, x, 1 - c, q)
    shifts = [(dx, dy) for dx in range(XS) for dy in range(YS) if (dx, dy) != (0, 0)]
    shifts.sort(key=lambda s: -(min(s[0], XS - s[0]) + min(s[1], YS - s[1])))
    steps = [d for k in range(NEAR, 0, -1) for d in (k, -k)]

    def rcopy(src, dst, ssem, rsem, where):
        return pltpu.make_async_remote_copy(
            src_ref=src, dst_ref=dst, send_sem=ssem, recv_sem=rsem,
            device_id=where, device_id_type=MESH)

    barrier = pltpu.get_barrier_semaphore()
    partners = [along(d) for d in steps] + [other]
    for dx, dy in shifts:
        xx, yy = plane(dx, dy)
        partners.append(dev(z, xx, c, yy))
    for where in partners:
        pl.semaphore_signal(barrier, inc=1, device_id=where, device_id_type=MESH)

    my_slots = (x * CORES + c) * CAP + 2 * q
    load_prev = pltpu.make_async_copy(prev_ref.at[pl.ds(2 * q, 2)], prev, loc.at[0])
    load_prev.start()

    owners = owner_ref[...]
    lanes = lax.broadcasted_iota(jnp.int32, (N, N), 1)
    subs = lax.broadcasted_iota(jnp.int32, (N, N), 0)
    rows = [jnp.broadcast_to(owners[h:h + 1, :], (N, N)) for h in range(2)]
    cols = [rows[h].T for h in range(2)]
    want = z * (XS * CORES * CAP) + lanes
    take = jnp.zeros((1, N), jnp.int32)
    filled = jnp.zeros((1, N), jnp.int32)
    n_plane = XS * CORES * CAP
    none_slot = 2 * CORES * zs
    for h in range(2):
        rank_c = jnp.zeros((N, 1), jnp.int32)
        rank_r = jnp.zeros((1, N), jnp.int32)
        for g in range(2):
            before = (cols[h] == rows[g]) & (lanes + N * g < subs + N * h)
            rank_c = rank_c + jnp.sum(before.astype(jnp.int32), axis=1, keepdims=True)
            after = (cols[g] == rows[h]) & (subs + N * g < lanes + N * h)
            rank_r = rank_r + jnp.sum(after.astype(jnp.int32), axis=0, keepdims=True)
        slot_c = cols[h] * CAP + rank_c
        slot_r = owners[h:h + 1, :] * CAP + rank_r
        blk = subs + N * h
        match = (slot_c == want) & (lanes < n_plane)
        place = (((blk >> 1) & 1) * zs + (blk >> 4)) * 2 + (blk & 1)
        here = match & (((blk >> 2) & 3) == x)
        take = take + jnp.sum(jnp.where(here, none_slot - place, 0), axis=0, keepdims=True)
        filled = filled + jnp.sum(match.astype(jnp.int32), axis=0, keepdims=True)
        back = jnp.where(slot_r >> 6 == z, slot_r & (n_plane - 1), n_plane)
        tabv[2 + h:3 + h, :] = back
    tabv[0:1, :] = none_slot - take
    tabv[1:2, :] = filled
    zeros = jnp.zeros((N // YS, N), BF)
    zbuf[none_slot] = zeros
    vbuf[n_plane] = zeros

    pl.semaphore_wait(barrier, len(partners))

    def zplace(cc, zz):
        return (cc * zs + zz) * 2

    sends = []
    zr = {}
    for d in steps:
        cp = rcopy(grad_ref, zbuf.at[pl.ds(zplace(c, z), 2)], z_send.at[len(sends)], z_recv.at[d + 7], along(d))
        cp.start()
        sends.append(cp)
    dcopies = []

    def to_other(src, zz, k):
        cp = rcopy(src, zbuf.at[pl.ds(zplace(c, zz), 2)], d_send.at[k], d_recv.at[k], other)
        cp.start()
        dcopies.append(cp)

    to_other(grad_ref, z, 0)
    tab_copy = pltpu.make_async_copy(tabv, tabs, loc.at[1])
    tab_copy.start()
    zbuf[pl.ds(zplace(c, z), 2)] = grad_ref[...]

    def arrived(d):
        ref = zbuf.at[pl.ds(zplace(c, zoff(-d)), 2)]
        rcopy(ref, ref, z_send.at[0], z_recv.at[d + 7], along(d)).wait_recv()

    for sgn in (1, -1):
        arrived(sgn * NEAR)
        src = zplace(c, zoff(-sgn * NEAR))
        half = zbuf.at[src + (0 if sgn > 0 else 1)]
        cp = rcopy(half, half, z_send.at[len(sends)], z_recv.at[15 if sgn > 0 else 16], along(sgn * NEAR))
        cp.start()
        sends.append(cp)
        whole = zbuf.at[pl.ds(src, 2)]
        for k in range(NEAR - 1, 0, -1):
            cp = rcopy(whole, whole, z_send.at[len(sends)], z_recv.at[sgn * (NEAR + k) + 7], along(sgn * k))
            cp.start()
            sends.append(cp)
    for k, d in enumerate([4, -4, 1, -1, 2, -2, 3, -3, 5, -5, 6, -6, 7, -7]):
        if abs(d) != NEAR:
            arrived(d)
        to_other(zbuf.at[pl.ds(zplace(c, zoff(-d)), 2)], zoff(-d), k + 1)
    for k in range(2):
        ref = zbuf.at[zplace(c, zoff(8)) + k]
        rcopy(ref, ref, z_send.at[0], z_recv.at[15 + k], other).wait_recv()
    to_other(zbuf.at[pl.ds(zplace(c, zoff(8)), 2)], zoff(8), 15)
    order = [0, 4, -4, 1, -1, 2, -2, 3, -3, 5, -5, 6, -6, 7, -7, 8]
    for k, d in enumerate(order):
        ref = zbuf.at[pl.ds(zplace(1 - c, zoff(-d)), 2)]
        rcopy(ref, ref, d_send.at[k], d_recv.at[k], other).wait_recv()

    tab_copy.wait()
    psends = []
    for i, (dx, dy) in enumerate([*shifts, (0, 0)]):
        xx, yy = plane(dx, dy)
        first = (xx * CORES + c) * CAP + 2 * yy
        if (dx, dy) != (0, 0):
            for r in range(2):
                sel1[i, r] = zbuf[tabs[0, first + r]]
            cp = rcopy(sel1.at[i], rbuf.at[x, q], p_send.at[i], p_recv.at[i], dev(z, xx, c, yy))
            cp.start()
            psends.append(cp)
        else:
            for r in range(2):
                rbuf[x, q, r] = zbuf[tabs[0, first + r]]
    for i, (dx, dy) in enumerate(shifts):
        ref = rbuf.at[lax.rem(x + XS - dx, XS), lax.rem(q + YS - dy, YS)]
        rcopy(ref, ref, p_send.at[i], p_recv.at[i], other).wait_recv()
    part = N // YS
    for r in range(2):
        for k in range(YS):
            total = rbuf[0, k, r] + rbuf[1, k, r] + rbuf[2, k, r] + rbuf[3, k, r]
            gt[r, part * k:part * (k + 1), :] = total

    load_prev.wait()
    eye = (lax.broadcasted_iota(jnp.int32, (N, N), 0) == lax.broadcasted_iota(jnp.int32, (N, N), 1)).astype(F32)
    for r in range(2):
        on = tabs[1, my_slots + r].astype(F32)
        g = gt[r]
        sides = [
            lax.dot_general(g, g, (((0,), (0,)), ((), ())), preferred_element_type=F32),
            lax.dot_general(g, g, (((1,), (1,)), ((), ())), preferred_element_type=F32),
        ]
        for k in range(2):
            blended = (STAT_DECAY * prev[r, k] + (1.0 - STAT_DECAY) * sides[k]) * on
            stat[r, k] = blended
            s = blended + (1.0 - on) * eye
            tr = jnp.sum(jnp.sum(s * eye, axis=1, keepdims=True), axis=0, keepdims=True)
            a = s + (DAMPING / N) * tr * eye
            norm = jnp.sqrt(jnp.sum(jnp.sum(a * a, axis=1, keepdims=True), axis=0, keepdims=True))
            xstate[2 * r + k] = eye * (1.0 / jnp.sqrt(jnp.sqrt(norm)))
            mstate[2 * r + k] = a * (1.0 / norm)

    ssends = []

    def share(src, dst_ref, ssem, rsem, lsem):
        mine = dst_ref.at[pl.ds(2 * q, 2)]
        keep = pltpu.make_async_copy(src, mine, lsem)
        keep.start()
        for dy in range(1, YS):
            cp = rcopy(src, mine, ssem.at[dy - 1], rsem.at[dy - 1], dev(z, x, c, lax.rem(q + dy, YS)))
            cp.start()
            ssends.append(cp)
        return keep

    keep_stat = share(stat, stats_ref, s_send, s_recv, loc.at[2])

    def body(it, unused):
        del it, unused
        fs, ms = [], []
        for p in range(4):
            m = mstate[p]
            fs.append(1.25 * eye - 0.25 * m)
            ms.append(wide(m))
        gs = []
        for p in range(4):
            w = wide(fs[p])
            right = jnp.concatenate([w, w], axis=0)
            gs.append(product(w, right))
            xstate[p] = product(wide(xstate[p]), right)
        rights = [tall(g) for g in gs]
        ts = [product(ms[p], rights[p]) for p in range(4)]
        for p in range(4):
            mstate[p] = product(wide(ts[p]), rights[p])
        return 0

    lax.fori_loop(0, ITERS - 1, body, 0)
    for r in range(2):
        on = tabs[1, my_slots + r].astype(F32)
        sides = []
        for k in range(2):
            f = 1.25 * eye - 0.25 * mstate[2 * r + k]
            sides.append(product(wide(xstate[2 * r + k]), tall(f)))
            root[r, k] = sides[k] * on
        g = gt[r]
        t = jnp.dot(wide(sides[1]), jnp.concatenate([g, g], axis=0), preferred_element_type=F32)
        pt = product(wide(t), tall(sides[0]))
        ms = jnp.sum(jnp.sum(pt * pt, axis=1, keepdims=True), axis=0, keepdims=True) * (1.0 / (N * N))
        spread = jnp.sqrt(ms) + (1.0 - on)
        u = (pt / spread).astype(BF)
        for k in range(YS):
            ubuf[k, r] = u[part * k:part * (k + 1), :]

    usends = []
    for i, (dx, dy) in enumerate([(0, 0), *shifts]):
        xx, yy = plane(dx, dy)
        if i == 0:
            vbuf[pl.ds(my_slots, 2)] = ubuf[q]
        else:
            cp = rcopy(ubuf.at[yy], vbuf.at[pl.ds(my_slots, 2)], u_send.at[i - 1], u_recv.at[i - 1], dev(z, xx, c, yy))
            cp.start()
            usends.append(cp)
    keep_root = share(root, roots_ref, r_send, r_recv, loc.at[3])
    for i, (dx, dy) in enumerate([(0, 0), *reversed(shifts)]):
        xx, yy = lax.rem(x + XS - dx, XS), lax.rem(q + YS - dy, YS)
        ref = vbuf.at[pl.ds((xx * CORES + c) * CAP + 2 * yy, 2)]
        if i == 0:
            src = ubuf.at[q]
        else:
            src = ref
            rcopy(ref, ref, u_send.at[0], u_recv.at[len(shifts) - i], other).wait_recv()
        cp = rcopy(src, ref, e_send.at[i], e_recv.at[i], other)
        cp.start()
        usends.append(cp)
    for i, (dx, dy) in enumerate([(0, 0), *reversed(shifts)]):
        xx, yy = lax.rem(x + XS - dx, XS), lax.rem(q + YS - dy, YS)
        ref = vbuf.at[pl.ds((xx * CORES + 1 - c) * CAP + 2 * yy, 2)]
        rcopy(ref, ref, e_send.at[i], e_recv.at[i], other).wait_recv()

    def chosen(d, i):
        b = ((zoff(d) * XS + x) * CORES + c) * 2 + i
        return vbuf[tabs[2 + lax.div(b, N), lax.rem(b, N)]]

    wsends = []

    def zsend(src, dst, k, d):
        cp = rcopy(src, dst, w_send.at[k], w_recv.at[k], along(d))
        cp.start()
        wsends.append(cp)

    for s, sgn in enumerate((1, -1)):
        wbuf[4 + s, 0] = chosen(8, s)
        zsend(wbuf.at[4 + s, 0], bfar.at[s, 3, 0], s * 4 + 3, sgn * NEAR)
        for k in range(NEAR - 1, 0, -1):
            for i in range(2):
                wbuf[6 + s * 3 + k - 1, i] = chosen(sgn * (NEAR + k), i)
            zsend(wbuf.at[6 + s * 3 + k - 1], bfar.at[s, k - 1], s * 4 + k - 1, sgn * k)
    for k in range(NEAR - 1, 0, -1):
        for s, sgn in enumerate((1, -1)):
            for i in range(2):
                wbuf[12 + s * 3 + k - 1, i] = chosen(sgn * k, i)
            zsend(wbuf.at[12 + s * 3 + k - 1], abuf.at[s, k - 1], 8 + s * 4 + k - 1, sgn * k)
    for s, sgn in enumerate((1, -1)):
        total = [chosen(sgn * NEAR, i) for i in range(2)]
        for k in range(1, NEAR + 1):
            ref = bfar.at[s, k - 1] if k < NEAR else bfar.at[s, 3, 0]
            rcopy(ref, ref, w_send.at[0], w_recv.at[s * 4 + k - 1], other).wait_recv()
            for i in range(2):
                if k < NEAR:
                    total[i] = total[i] + bfar[s, k - 1, i]
                elif i == s:
                    total[i] = total[i] + bfar[s, 3, 0]
        for i in range(2):
            mfar[s, i] = total[i]
        zsend(mfar.at[s], abuf.at[s, 3], 8 + s * 4 + 3, sgn * NEAR)
    total = [chosen(0, i) for i in range(2)]
    for k in range(1, NEAR + 1):
        for s in range(2):
            ref = abuf.at[s, k - 1]
            rcopy(ref, ref, w_send.at[0], w_recv.at[8 + s * 4 + k - 1], other).wait_recv()
            for i in range(2):
                total[i] = total[i] + abuf[s, k - 1, i]
    for i in range(2):
        upd_ref[i] = total[i]

    for rsem, ref in ((s_recv, stats_ref), (r_recv, roots_ref)):
        for dy in range(1, YS):
            dst = ref.at[pl.ds(2 * lax.rem(q + YS - dy, YS), 2)]
            rcopy(dst, dst, s_send.at[0], rsem.at[dy - 1], other).wait_recv()
    keep_stat.wait()
    keep_root.wait()
    for cp in sends + dcopies + psends + ssends + usends + wsends:
        cp.wait_send()


def per_device(grad_blocks, owner_table, prev_stats):
    zs = lax.axis_size("dp") // (XS * CORES)
    gt = jnp.swapaxes(grad_blocks, 1, 2)
    part = N // YS
    dma = pltpu.SemaphoreType.DMA
    n_shift = XS * YS - 1
    upd, stats, roots = pl.pallas_call(
        lambda *refs: kernel(zs, *refs),
        out_shape=(
            jax.ShapeDtypeStruct((2, part, N), BF),
            jax.ShapeDtypeStruct(prev_stats.shape, F32),
            jax.ShapeDtypeStruct(prev_stats.shape, F32),
        ),
        in_specs=[
            pl.BlockSpec(memory_space=pltpu.VMEM),
            pl.BlockSpec(memory_space=pltpu.VMEM),
            pl.BlockSpec(memory_space=pl.ANY),
        ],
        out_specs=(
            pl.BlockSpec(memory_space=pltpu.VMEM),
            pl.BlockSpec(memory_space=pl.ANY),
            pl.BlockSpec(memory_space=pl.ANY),
        ),
        scratch_shapes=[
            pltpu.VMEM((2 * CORES * zs + 1, part, N), BF),
            pltpu.VMEM((n_shift, 2, part, N), BF),
            pltpu.VMEM((XS, YS, 2, part, N), BF),
            pltpu.VMEM((2, N, N), BF),
            pltpu.VMEM((2, 2, N, N), F32),
            pltpu.VMEM((2, 2, N, N), F32),
            pltpu.VMEM((2, 2, N, N), F32),
            pltpu.VMEM((4, N, N), F32),
            pltpu.VMEM((4, N, N), F32),
            pltpu.VMEM((YS, 2, part, N), BF),
            pltpu.VMEM((XS * CORES * CAP + 1, part, N), BF),
            pltpu.VMEM((18, 2, part, N), BF),
            pltpu.VMEM((2, 4, 2, part, N), BF),
            pltpu.VMEM((2, 2, part, N), BF),
            pltpu.VMEM((2, 4, 2, part, N), BF),
            pltpu.VMEM((8, N), jnp.int32),
            pltpu.SMEM((8, N), jnp.int32),
            dma((16,)), dma((17,)),
            dma((16,)), dma((16,)),
            dma((n_shift,)), dma((n_shift,)),
            dma((3,)), dma((3,)), dma((3,)), dma((3,)),
            dma((n_shift,)), dma((n_shift,)),
            dma((16,)), dma((16,)),
            dma((16,)), dma((16,)),
            dma((4,)),
        ],
        compiler_params=pltpu.CompilerParams(
            collective_id=0, has_side_effects=True, vmem_limit_bytes=32 * 1024 * 1024),
    )(gt, owner_table.reshape(2, N), prev_stats)
    return jnp.swapaxes(upd, 1, 2), stats, roots


def solution(mesh):
    return jax.shard_map(
        per_device,
        mesh=mesh,
        in_specs=(P("dp", None, "mp"), P(), P("dp", None, None, None)),
        out_specs=(P("dp", None, "mp"), P("dp", None, None, None), P("dp", None, None, None)),
        check_vma=False,
    )
```

```python
import jax
import jax.numpy as jnp
from jax import lax
from jax.experimental import pallas as pl
from jax.experimental.pallas import tpu as pltpu
from jax.sharding import PartitionSpec as P

ITERS = 16
STAT_DECAY = 0.75
DAMPING = 0.03
N = 128
XS, CORES, YS = 4, 2, 4
CAP = 8
NEAR = 4
MESH = pl.DeviceIdType.MESH
BF = jnp.bfloat16
F32 = jnp.float32


def split(a):
    hi = a.astype(BF)
    return hi, (a - hi.astype(F32)).astype(BF)


def wide(a):
    return jnp.concatenate(split(a), axis=1)


def tall(a):
    row = wide(a)
    return jnp.concatenate([row, row], axis=0)


def product(left, right):
    out = jnp.dot(left, right, preferred_element_type=F32)
    return out[:, :N] + out[:, N:]


def kernel(
    zs,
    grad_hbm, owner_hbm, prev_ref,
    upd_ref, stats_ref, roots_ref,
    zbuf, sel1, rbuf, gt, prev, stat, root, mstate, xstate, ubuf, vbuf, wbuf, bfar, mfar, abuf, tabv, tabs, grad_ref, owner_ref,
    z_send, z_recv, d_send, d_recv, p_send, p_recv, s_send, s_recv, r_send, r_recv,
    u_send, u_recv, e_send, e_recv, w_send, w_recv, loc,
):
    dp = lax.axis_index("dp")
    q = lax.axis_index("mp")
    z = lax.div(dp, XS * CORES)
    x = lax.rem(lax.div(dp, CORES), XS)
    c = lax.rem(dp, CORES)

    load_owner = pltpu.make_async_copy(owner_hbm, owner_ref, loc.at[1])
    load_owner.start()
    load_grad = pltpu.make_async_copy(grad_hbm, grad_ref, loc.at[2])
    load_grad.start()

    def zoff(d):
        return lax.rem(z + (d + zs), zs)

    def dev(zz, xx, cc, yy):
        return ((zz * XS + xx) * CORES + cc, yy)

    def along(d):
        return dev(zoff(d), x, c, q)

    def plane(dx, dy):
        return lax.rem(x + dx, XS), lax.rem(q + dy, YS)

    other = dev(z, x, 1 - c, q)
    shifts = [(dx, dy) for dx in range(XS) for dy in range(YS) if (dx, dy) != (0, 0)]
    shifts.sort(key=lambda s: -(min(s[0], XS - s[0]) + min(s[1], YS - s[1])))
    steps = [d for k in range(NEAR, 0, -1) for d in (k, -k)]

    def rcopy(src, dst, ssem, rsem, where):
        return pltpu.make_async_remote_copy(
            src_ref=src, dst_ref=dst, send_sem=ssem, recv_sem=rsem,
            device_id=where, device_id_type=MESH)

    barrier = pltpu.get_barrier_semaphore()
    partners = [along(d) for d in steps] + [other]
    for dx, dy in shifts:
        xx, yy = plane(dx, dy)
        partners.append(dev(z, xx, c, yy))
    for where in partners:
        pl.semaphore_signal(barrier, inc=1, device_id=where, device_id_type=MESH)

    my_slots = (x * CORES + c) * CAP + 2 * q
    load_prev = pltpu.make_async_copy(prev_ref.at[pl.ds(2 * q, 2)], prev, loc.at[0])
    load_prev.start()

    load_owner.wait()
    owners = owner_ref[...]
    lanes = lax.broadcasted_iota(jnp.int32, (N, N), 1)
    subs = lax.broadcasted_iota(jnp.int32, (N, N), 0)
    rows = [jnp.broadcast_to(owners[h:h + 1, :], (N, N)) for h in range(2)]
    cols = [rows[h].T for h in range(2)]
    want = z * (XS * CORES * CAP) + lanes
    take = jnp.zeros((1, N), jnp.int32)
    filled = jnp.zeros((1, N), jnp.int32)
    n_plane = XS * CORES * CAP
    none_slot = 2 * CORES * zs
    for h in range(2):
        rank_c = jnp.zeros((N, 1), jnp.int32)
        rank_r = jnp.zeros((1, N), jnp.int32)
        for g in range(2):
            before = (cols[h] == rows[g]) & (lanes + N * g < subs + N * h)
            rank_c = rank_c + jnp.sum(before.astype(jnp.int32), axis=1, keepdims=True)
            after = (cols[g] == rows[h]) & (subs + N * g < lanes + N * h)
            rank_r = rank_r + jnp.sum(after.astype(jnp.int32), axis=0, keepdims=True)
        slot_c = cols[h] * CAP + rank_c
        slot_r = owners[h:h + 1, :] * CAP + rank_r
        blk = subs + N * h
        match = (slot_c == want) & (lanes < n_plane)
        place = (((blk >> 1) & 1) * zs + (blk >> 4)) * 2 + (blk & 1)
        here = match & (((blk >> 2) & 3) == x)
        take = take + jnp.sum(jnp.where(here, none_slot - place, 0), axis=0, keepdims=True)
        filled = filled + jnp.sum(match.astype(jnp.int32), axis=0, keepdims=True)
        back = jnp.where(slot_r >> 6 == z, slot_r & (n_plane - 1), n_plane)
        tabv[2 + h:3 + h, :] = back
    tabv[0:1, :] = none_slot - take
    tabv[1:2, :] = filled
    zeros = jnp.zeros((N // YS, N), BF)
    zbuf[none_slot] = zeros
    vbuf[n_plane] = zeros

    load_grad.wait()
    pl.semaphore_wait(barrier, len(partners))

    def zplace(cc, zz):
        return (cc * zs + zz) * 2

    sends = []
    zr = {}
    for d in steps:
        cp = rcopy(grad_ref, zbuf.at[pl.ds(zplace(c, z), 2)], z_send.at[len(sends)], z_recv.at[d + 7], along(d))
        cp.start()
        sends.append(cp)
    dcopies = []

    def to_other(src, zz, k):
        cp = rcopy(src, zbuf.at[pl.ds(zplace(c, zz), 2)], d_send.at[k], d_recv.at[k], other)
        cp.start()
        dcopies.append(cp)

    to_other(grad_ref, z, 0)
    tab_copy = pltpu.make_async_copy(tabv, tabs, loc.at[1])
    tab_copy.start()
    zbuf[pl.ds(zplace(c, z), 2)] = grad_ref[...]

    def arrived(d):
        ref = zbuf.at[pl.ds(zplace(c, zoff(-d)), 2)]
        rcopy(ref, ref, z_send.at[0], z_recv.at[d + 7], along(d)).wait_recv()

    for sgn in (1, -1):
        arrived(sgn * NEAR)
        src = zplace(c, zoff(-sgn * NEAR))
        half = zbuf.at[src + (0 if sgn > 0 else 1)]
        cp = rcopy(half, half, z_send.at[len(sends)], z_recv.at[15 if sgn > 0 else 16], along(sgn * NEAR))
        cp.start()
        sends.append(cp)
        whole = zbuf.at[pl.ds(src, 2)]
        for k in range(NEAR - 1, 0, -1):
            cp = rcopy(whole, whole, z_send.at[len(sends)], z_recv.at[sgn * (NEAR + k) + 7], along(sgn * k))
            cp.start()
            sends.append(cp)
    for k, d in enumerate([4, -4, 1, -1, 2, -2, 3, -3, 5, -5, 6, -6, 7, -7]):
        if abs(d) != NEAR:
            arrived(d)
        to_other(zbuf.at[pl.ds(zplace(c, zoff(-d)), 2)], zoff(-d), k + 1)
    for k in range(2):
        ref = zbuf.at[zplace(c, zoff(8)) + k]
        rcopy(ref, ref, z_send.at[0], z_recv.at[15 + k], other).wait_recv()
    to_other(zbuf.at[pl.ds(zplace(c, zoff(8)), 2)], zoff(8), 15)
    order = [0, 4, -4, 1, -1, 2, -2, 3, -3, 5, -5, 6, -6, 7, -7, 8]
    for k, d in enumerate(order):
        ref = zbuf.at[pl.ds(zplace(1 - c, zoff(-d)), 2)]
        rcopy(ref, ref, d_send.at[k], d_recv.at[k], other).wait_recv()

    tab_copy.wait()
    psends = []
    for i, (dx, dy) in enumerate([*shifts, (0, 0)]):
        xx, yy = plane(dx, dy)
        first = (xx * CORES + c) * CAP + 2 * yy
        if (dx, dy) != (0, 0):
            for r in range(2):
                sel1[i, r] = zbuf[tabs[0, first + r]]
            cp = rcopy(sel1.at[i], rbuf.at[x, q], p_send.at[i], p_recv.at[i], dev(z, xx, c, yy))
            cp.start()
            psends.append(cp)
        else:
            for r in range(2):
                rbuf[x, q, r] = zbuf[tabs[0, first + r]]
    for i, (dx, dy) in enumerate(shifts):
        ref = rbuf.at[lax.rem(x + XS - dx, XS), lax.rem(q + YS - dy, YS)]
        rcopy(ref, ref, p_send.at[i], p_recv.at[i], other).wait_recv()
    part = N // YS
    for r in range(2):
        for k in range(YS):
            total = rbuf[0, k, r] + rbuf[1, k, r] + rbuf[2, k, r] + rbuf[3, k, r]
            gt[r, part * k:part * (k + 1), :] = total

    load_prev.wait()
    eye = (lax.broadcasted_iota(jnp.int32, (N, N), 0) == lax.broadcasted_iota(jnp.int32, (N, N), 1)).astype(F32)
    for r in range(2):
        on = tabs[1, my_slots + r].astype(F32)
        g = gt[r]
        sides = [
            lax.dot_general(g, g, (((0,), (0,)), ((), ())), preferred_element_type=F32),
            lax.dot_general(g, g, (((1,), (1,)), ((), ())), preferred_element_type=F32),
        ]
        for k in range(2):
            blended = (STAT_DECAY * prev[r, k] + (1.0 - STAT_DECAY) * sides[k]) * on
            stat[r, k] = blended
            s = blended + (1.0 - on) * eye
            tr = jnp.sum(jnp.sum(s * eye, axis=1, keepdims=True), axis=0, keepdims=True)
            a = s + (DAMPING / N) * tr * eye
            norm = jnp.sqrt(jnp.sum(jnp.sum(a * a, axis=1, keepdims=True), axis=0, keepdims=True))
            xstate[2 * r + k] = eye * (1.0 / jnp.sqrt(jnp.sqrt(norm)))
            mstate[2 * r + k] = a * (1.0 / norm)

    ssends = []

    def share(src, dst_ref, ssem, rsem, lsem):
        mine = dst_ref.at[pl.ds(2 * q, 2)]
        keep = pltpu.make_async_copy(src, mine, lsem)
        keep.start()
        for dy in range(1, YS):
            cp = rcopy(src, mine, ssem.at[dy - 1], rsem.at[dy - 1], dev(z, x, c, lax.rem(q + dy, YS)))
            cp.start()
            ssends.append(cp)
        return keep

    keep_stat = share(stat, stats_ref, s_send, s_recv, loc.at[2])

    def body(it, unused):
        del it, unused
        fs, ms = [], []
        for p in range(4):
            m = mstate[p]
            fs.append(1.25 * eye - 0.25 * m)
            ms.append(wide(m))
        gs = []
        for p in range(4):
            w = wide(fs[p])
            right = jnp.concatenate([w, w], axis=0)
            gs.append(product(w, right))
            xstate[p] = product(wide(xstate[p]), right)
        rights = [tall(g) for g in gs]
        ts = [product(ms[p], rights[p]) for p in range(4)]
        for p in range(4):
            mstate[p] = product(wide(ts[p]), rights[p])
        return 0

    lax.fori_loop(0, ITERS - 1, body, 0)
    for r in range(2):
        on = tabs[1, my_slots + r].astype(F32)
        sides = []
        for k in range(2):
            f = 1.25 * eye - 0.25 * mstate[2 * r + k]
            sides.append(product(wide(xstate[2 * r + k]), tall(f)))
            root[r, k] = sides[k] * on
        g = gt[r]
        t = jnp.dot(wide(sides[1]), jnp.concatenate([g, g], axis=0), preferred_element_type=F32)
        pt = product(wide(t), tall(sides[0]))
        ms = jnp.sum(jnp.sum(pt * pt, axis=1, keepdims=True), axis=0, keepdims=True) * (1.0 / (N * N))
        spread = jnp.sqrt(ms) + (1.0 - on)
        u = (pt / spread).astype(BF)
        for k in range(YS):
            ubuf[k, r] = u[part * k:part * (k + 1), :]

    usends = []
    for i, (dx, dy) in enumerate([(0, 0), *shifts]):
        xx, yy = plane(dx, dy)
        if i == 0:
            vbuf[pl.ds(my_slots, 2)] = ubuf[q]
        else:
            cp = rcopy(ubuf.at[yy], vbuf.at[pl.ds(my_slots, 2)], u_send.at[i - 1], u_recv.at[i - 1], dev(z, xx, c, yy))
            cp.start()
            usends.append(cp)
    keep_root = share(root, roots_ref, r_send, r_recv, loc.at[3])
    for i, (dx, dy) in enumerate([(0, 0), *reversed(shifts)]):
        xx, yy = lax.rem(x + XS - dx, XS), lax.rem(q + YS - dy, YS)
        ref = vbuf.at[pl.ds((xx * CORES + c) * CAP + 2 * yy, 2)]
        if i == 0:
            src = ubuf.at[q]
        else:
            src = ref
            rcopy(ref, ref, u_send.at[0], u_recv.at[len(shifts) - i], other).wait_recv()
        cp = rcopy(src, ref, e_send.at[i], e_recv.at[i], other)
        cp.start()
        usends.append(cp)
    for i, (dx, dy) in enumerate([(0, 0), *reversed(shifts)]):
        xx, yy = lax.rem(x + XS - dx, XS), lax.rem(q + YS - dy, YS)
        ref = vbuf.at[pl.ds((xx * CORES + 1 - c) * CAP + 2 * yy, 2)]
        rcopy(ref, ref, e_send.at[i], e_recv.at[i], other).wait_recv()

    def chosen(d, i):
        b = ((zoff(d) * XS + x) * CORES + c) * 2 + i
        return vbuf[tabs[2 + lax.div(b, N), lax.rem(b, N)]]

    wsends = []

    def zsend(src, dst, k, d):
        cp = rcopy(src, dst, w_send.at[k], w_recv.at[k], along(d))
        cp.start()
        wsends.append(cp)

    for s, sgn in enumerate((1, -1)):
        wbuf[4 + s, 0] = chosen(8, s)
        zsend(wbuf.at[4 + s, 0], bfar.at[s, 3, 0], s * 4 + 3, sgn * NEAR)
        for k in range(NEAR - 1, 0, -1):
            for i in range(2):
                wbuf[6 + s * 3 + k - 1, i] = chosen(sgn * (NEAR + k), i)
            zsend(wbuf.at[6 + s * 3 + k - 1], bfar.at[s, k - 1], s * 4 + k - 1, sgn * k)
    for k in range(NEAR - 1, 0, -1):
        for s, sgn in enumerate((1, -1)):
            for i in range(2):
                wbuf[12 + s * 3 + k - 1, i] = chosen(sgn * k, i)
            zsend(wbuf.at[12 + s * 3 + k - 1], abuf.at[s, k - 1], 8 + s * 4 + k - 1, sgn * k)
    for s, sgn in enumerate((1, -1)):
        total = [chosen(sgn * NEAR, i) for i in range(2)]
        for k in range(1, NEAR + 1):
            ref = bfar.at[s, k - 1] if k < NEAR else bfar.at[s, 3, 0]
            rcopy(ref, ref, w_send.at[0], w_recv.at[s * 4 + k - 1], other).wait_recv()
            for i in range(2):
                if k < NEAR:
                    total[i] = total[i] + bfar[s, k - 1, i]
                elif i == s:
                    total[i] = total[i] + bfar[s, 3, 0]
        for i in range(2):
            mfar[s, i] = total[i]
        zsend(mfar.at[s], abuf.at[s, 3], 8 + s * 4 + 3, sgn * NEAR)
    total = [chosen(0, i) for i in range(2)]
    for k in range(1, NEAR + 1):
        for s in range(2):
            ref = abuf.at[s, k - 1]
            rcopy(ref, ref, w_send.at[0], w_recv.at[8 + s * 4 + k - 1], other).wait_recv()
            for i in range(2):
                total[i] = total[i] + abuf[s, k - 1, i]
    for i in range(2):
        upd_ref[i] = total[i]

    for rsem, ref in ((s_recv, stats_ref), (r_recv, roots_ref)):
        for dy in range(1, YS):
            dst = ref.at[pl.ds(2 * lax.rem(q + YS - dy, YS), 2)]
            rcopy(dst, dst, s_send.at[0], rsem.at[dy - 1], other).wait_recv()
    keep_stat.wait()
    keep_root.wait()
    for cp in sends + dcopies + psends + ssends + usends + wsends:
        cp.wait_send()


def per_device(grad_blocks, owner_table, prev_stats):
    zs = lax.axis_size("dp") // (XS * CORES)
    gt = jnp.swapaxes(grad_blocks, 1, 2)
    part = N // YS
    dma = pltpu.SemaphoreType.DMA
    n_shift = XS * YS - 1
    upd, stats, roots = pl.pallas_call(
        lambda *refs: kernel(zs, *refs),
        out_shape=(
            jax.ShapeDtypeStruct((2, part, N), BF),
            jax.ShapeDtypeStruct(prev_stats.shape, F32),
            jax.ShapeDtypeStruct(prev_stats.shape, F32),
        ),
        in_specs=[
            pl.BlockSpec(memory_space=pltpu.HBM),
            pl.BlockSpec(memory_space=pltpu.HBM),
            pl.BlockSpec(memory_space=pltpu.HBM),
        ],
        out_specs=(
            pl.BlockSpec(memory_space=pltpu.VMEM),
            pl.BlockSpec(memory_space=pltpu.VMEM),
            pl.BlockSpec(memory_space=pltpu.VMEM),
        ),
        scratch_shapes=[
            pltpu.VMEM((2 * CORES * zs + 1, part, N), BF),
            pltpu.VMEM((n_shift, 2, part, N), BF),
            pltpu.VMEM((XS, YS, 2, part, N), BF),
            pltpu.VMEM((2, N, N), BF),
            pltpu.VMEM((2, 2, N, N), F32),
            pltpu.VMEM((2, 2, N, N), F32),
            pltpu.VMEM((2, 2, N, N), F32),
            pltpu.VMEM((4, N, N), F32),
            pltpu.VMEM((4, N, N), F32),
            pltpu.VMEM((YS, 2, part, N), BF),
            pltpu.VMEM((XS * CORES * CAP + 1, part, N), BF),
            pltpu.VMEM((18, 2, part, N), BF),
            pltpu.VMEM((2, 4, 2, part, N), BF),
            pltpu.VMEM((2, 2, part, N), BF),
            pltpu.VMEM((2, 4, 2, part, N), BF),
            pltpu.VMEM((8, N), jnp.int32),
            pltpu.SMEM((8, N), jnp.int32),
            pltpu.VMEM((2, part, N), BF),
            pltpu.VMEM((2, N), jnp.int32),
            dma((16,)), dma((17,)),
            dma((16,)), dma((16,)),
            dma((n_shift,)), dma((n_shift,)),
            dma((3,)), dma((3,)), dma((3,)), dma((3,)),
            dma((n_shift,)), dma((n_shift,)),
            dma((16,)), dma((16,)),
            dma((16,)), dma((16,)),
            dma((4,)),
        ],
        compiler_params=pltpu.CompilerParams(
            collective_id=0, has_side_effects=True, vmem_limit_bytes=40 * 1024 * 1024),
    )(*[pltpu.with_memory_space_constraint(a, pltpu.HBM) for a in (gt, owner_table.reshape(2, N), prev_stats)])
    upd, stats, roots = write_out(upd, stats, roots)
    return jnp.swapaxes(upd, 1, 2), stats, roots


def write_kernel(*refs):
    ins, outs, sems = refs[:3], refs[3:6], refs[6]
    copies = [pltpu.make_async_copy(ins[k], outs[k], sems.at[k]) for k in range(3)]
    for cp in copies:
        cp.start()
    for cp in copies:
        cp.wait()


def write_out(*arrays):
    return pl.pallas_call(
        write_kernel,
        out_shape=tuple(jax.ShapeDtypeStruct(a.shape, a.dtype) for a in arrays),
        in_specs=[pl.BlockSpec(memory_space=pltpu.VMEM)] * 3,
        out_specs=(pl.BlockSpec(memory_space=pltpu.HBM),) * 3,
        scratch_shapes=[pltpu.SemaphoreType.DMA((3,))],
        compiler_params=pltpu.CompilerParams(vmem_limit_bytes=16 * 1024 * 1024),
    )(*arrays)


def solution(mesh):
    return jax.shard_map(
        per_device,
        mesh=mesh,
        in_specs=(P("dp", None, "mp"), P(), P("dp", None, None, None)),
        out_specs=(P("dp", None, "mp"), P("dp", None, None, None), P("dp", None, None, None)),
        check_vma=False,
    )
```
